32 devices in a mesh: grp: 2 (over y), seq: 4 (over z), head: 2 (over x), sub: 2 (over core).
Axes of the slice: x: 2, y: 2, z: 4, core: 2. Of those that a mesh axis runs over, the one named last changes fastest.
Arguments:
- latents: bfloat16 [8, 256, 1152], P(('grp', 'seq'), ('head', 'sub')), parts along dimension 0, may hold values from -6 to 6
- timestep: int32 [2], P('grp'), parts along dimension 0, may hold values from 0 to 29
- time_table: float32 [30, 3, 1152], replicated, may hold values from -3 to 3
- shift_table: float32 [2, 3, 1152], replicated, may hold values from -2 to 2
- qkv_weight: bfloat16 [2, 1152, 16, 216], P(None, None, ('head', 'sub')), may hold values from -0.1875 to 0.1875
- norm_gains: float32 [2, 2, 72], replicated, may hold values from 0.1 to 1.9
- out_weight: bfloat16 [2, 1152, 1152], P(None, ('head', 'sub')), may hold values from -0.1875 to 0.1875
Outputs:
- mixed: bfloat16 [8, 256, 1152], P(('grp', 'seq'), ('head', 'sub')), parts along dimension 0
The draws below stay inside these ranges and needn't reach their ends.
There are 2 independent parts, one for each index of `grp`. The reference program is written for one: setup_inputs(seed, part) draws one part's arguments, and reference() takes and returns one part's arrays. A program takes and returns all parts, laid end to end along the dimension named above; an argument that names none is the same for every part. Nothing has to cross between parts.
All inputs are finite; a program needn't handle non-finite values.
Results may differ from the reference program's by a relative error of at most 0.0095.
Values may be sent and summed in bfloat16 or wider, within the bound.
No kernel may reach another device: no remote copies, remote signals or barrier semaphores. Data moves between devices by JAX's collectives and lax.ppermute only.
A program may use at most 64 MiB of HBM per device.

```python
import jax
import jax.numpy as jnp
from jax import lax

D = 1152
HEADS = 16
HEAD_DIM = 72
STEPS = 30
FRAMES = 4
PIX = 256
N_HEAD = 2
N_SUB = 2


def steps_of(stream_key, shape, split, smallest, largest):
    loudness = 1.0
    for position, parts in split:
        draws = jax.random.uniform(jax.random.fold_in(jax.random.fold_in(stream_key, 6), position), (parts,), jnp.float32, smallest / len(split), largest / len(split))
        loudness = loudness * jnp.repeat(jnp.exp(draws), shape[position] // parts).reshape((-1,) + (1,) * (len(shape) - 1 - position))
    return loudness


def scatter_about(stream_key, shape, scale, reach, shards=(), kind=jnp.bfloat16):
    entries = scale * jax.random.normal(stream_key, shape, jnp.float32)
    if shards:
        entries = entries * steps_of(stream_key, shape, shards, -0.22, 0.18)
    return jnp.clip(entries, -reach, reach).astype(kind)


def setup_inputs(seed: int = 0, part: int = 0) -> dict:
    keys = jax.random.split(jax.random.key(seed), 8)
    own_keys = jax.random.split(jax.random.fold_in(keys[7], part), 8)
    latents = scatter_about(own_keys[0], (FRAMES, PIX, D), 1.0, 6.0, ((0, 4), (1, 4)))
    timestep = jax.random.randint(own_keys[1], (1,), 0, STEPS).astype(jnp.int32)
    time_table = scatter_about(keys[2], (STEPS, 3, D), 0.5, 3.0, (), jnp.float32)
    shift_table = scatter_about(keys[3], (2, 3, D), 0.3, 2.0, (), jnp.float32)
    qkv_weight = scatter_about(keys[4], (2, D, HEADS, 3 * HEAD_DIM), D ** -0.5, 0.1875, ((2, 4),))
    norm_gains = jnp.clip(1.0 + 0.18 * jax.random.normal(keys[5], (2, 2, HEAD_DIM), jnp.float32), 0.1, 1.9)
    out_weight = scatter_about(keys[6], (2, D, D), D ** -0.5, 0.1875, ((1, 4),))
    return {"latents": latents, "timestep": timestep, "time_table": time_table, "shift_table": shift_table, "qkv_weight": qkv_weight, "norm_gains": norm_gains, "out_weight": out_weight}


EPSILON = 1e-06

def modulate(values, shift_row, scale_row):
    widened = values.astype(jnp.float32)
    center = lax.optimization_barrier(jnp.mean(widened, axis=-1, keepdims=True))
    spread = lax.optimization_barrier(jnp.mean(jnp.square(widened - center), axis=-1, keepdims=True))
    normal = (widened - center) * lax.rsqrt(spread + EPSILON)
    return (normal * (1.0 + scale_row) + shift_row).astype(jnp.bfloat16)

def rms_gain(values, gain_row):
    return values * lax.rsqrt(lax.optimization_barrier(jnp.mean(jnp.square(values), axis=-1, keepdims=True)) + EPSILON) * gain_row

def project(normed, weight, gain_pair):
    leading = normed.shape[:-1]
    head_count = weight.shape[1]
    head_dim = weight.shape[2] // 3
    flattened = jnp.dot(normed.reshape(-1, normed.shape[-1]), weight.reshape(weight.shape[0], -1), preferred_element_type=jnp.float32)
    pieces = flattened.reshape(leading + (head_count, 3, head_dim))
    queries = rms_gain(pieces[..., 0, :], gain_pair[0])
    key_part = rms_gain(pieces[..., 1, :], gain_pair[1])
    return jnp.concatenate([queries, key_part, pieces[..., 2, :]], axis=-1).astype(jnp.bfloat16)

def attend(packed):
    head_dim = packed.shape[-1] // 3
    queries = packed[..., :head_dim].astype(jnp.float32)
    key_part = packed[..., head_dim:2 * head_dim].astype(jnp.float32)
    value_part = packed[..., 2 * head_dim:].astype(jnp.float32)
    scores = jnp.einsum('qhd,khd->hqk', queries, key_part) * head_dim ** (-0.5)
    exponent = jnp.exp(scores)
    weights = (exponent / lax.optimization_barrier(jnp.sum(exponent, axis=-1, keepdims=True))).astype(jnp.bfloat16)
    return jnp.einsum('hqk,khd->qhd', weights.astype(jnp.float32), value_part).astype(jnp.bfloat16)

def finish(attended, residual, out_matrix, gate_row):
    flat_rows = attended.reshape(-1, out_matrix.shape[0])
    update = jnp.dot(flat_rows, out_matrix, preferred_element_type=jnp.float32)
    update = update.reshape(residual.shape)
    return (residual.astype(jnp.float32) + gate_row * update).astype(jnp.bfloat16)

def reference(latents, timestep, time_table, shift_table, qkv_weight, norm_gains, out_weight):
    modulation = time_table[timestep[0]][None] + shift_table

    def spatial_frame(frame):
        normed = modulate(frame, modulation[0, 0], modulation[0, 1])
        packed = project(normed, qkv_weight[0], norm_gains[0])
        attended = attend(packed)
        return finish(attended, frame, out_weight[0], modulation[0, 2])
    current = lax.map(spatial_frame, latents)
    frame_count, pixel_count, feature_width = current.shape
    block_count = N_HEAD * N_SUB
    slabs = current.reshape(frame_count, block_count, pixel_count // block_count, feature_width)
    slabs = jnp.moveaxis(slabs, 1, 0)

    def temporal_slab(slab):
        normed = modulate(slab, modulation[1, 0], modulation[1, 1])
        packed = project(normed, qkv_weight[1], norm_gains[1])
        attended = jax.vmap(attend, in_axes=1, out_axes=1)(packed)
        return finish(attended, slab, out_weight[1], modulation[1, 2])
    mixed = lax.map(temporal_slab, slabs)
    mixed = jnp.moveaxis(mixed, 0, 1).reshape(frame_count, pixel_count, feature_width)
    return mixed
```

```python
import functools

import jax
import jax.numpy as jnp
from jax import lax
from jax.experimental import pallas as pl
from jax.experimental.pallas import tpu as pltpu
from jax.sharding import PartitionSpec as P

EPSILON = 1e-06
F32 = jnp.float32
BF16 = jnp.bfloat16
VMEM = pl.BlockSpec(memory_space=pltpu.VMEM)
SMEM = pl.BlockSpec(memory_space=pltpu.SMEM)
HBM = pl.BlockSpec(memory_space=pltpu.HBM)


def call(kernel, name, out_shape, in_specs, scratch=(), flops=0, moved=0, limit=24):
    return pl.pallas_call(
        kernel,
        name=name,
        out_shape=out_shape,
        in_specs=in_specs,
        out_specs=jax.tree.map(lambda _: VMEM, out_shape),
        scratch_shapes=list(scratch),
        compiler_params=pltpu.CompilerParams(vmem_limit_bytes=limit * 1024 * 1024),
        cost_estimate=pl.CostEstimate(flops=flops, bytes_accessed=moved, transcendentals=0),
    )


def layer_norm(rows, shift_row, scale_row):
    wide = rows.astype(F32)
    center = jnp.mean(wide, axis=-1, keepdims=True)
    moved = wide - center
    spread = jnp.mean(moved * moved, axis=-1, keepdims=True)
    return (moved * lax.rsqrt(spread + EPSILON) * (1.0 + scale_row) + shift_row).astype(BF16)


def project(normed, weight, gain_q, gain_k, heads):
    flat = lax.dot_general(weight, normed, (((1,), (1,)), ((), ())), preferred_element_type=F32)
    dim = flat.shape[0] // (3 * heads)
    pieces = []
    for head in range(heads):
        for part, gain in ((0, gain_q), (1, gain_k), (2, None)):
            start = (3 * head + part) * dim
            values = flat[start : start + dim]
            if gain is not None:
                power = jnp.mean(values * values, axis=0, keepdims=True)
                values = values * lax.rsqrt(power + EPSILON) * gain
            pieces.append(values.astype(BF16))
    return pieces


def attend(queries, keys, values, mask):
    dim = queries.shape[0]
    scores = lax.dot_general(keys, queries, (((0,), (0,)), ((), ())), preferred_element_type=F32)
    weights = jnp.exp(scores * dim ** (-0.5))
    if mask is not None:
        weights = weights * mask
    total = jnp.sum(weights, axis=0, keepdims=True)
    mixed = jnp.dot(values, weights.astype(BF16), preferred_element_type=F32)
    return mixed / total


def first_kernel(sizes, step_ref, table_ref, shift_ref, own_ref, pair_ref, gain_ref, qkv_hbm, out_hbm,
                 mod_ref, packed_ref, qkv0_ref, qkv1_ref, out0_ref, out1_ref, sems):
    heads, rows, dim = sizes
    copies = [
        pltpu.make_async_copy(source.at[layer], target, sems.at[i])
        for i, (source, layer, target) in enumerate(
            ((qkv_hbm, 0, qkv0_ref), (out_hbm, 0, out0_ref), (qkv_hbm, 1, qkv1_ref), (out_hbm, 1, out1_ref))
        )
    ]
    for copy in copies:
        copy.start()
    step = step_ref[0]
    for j in range(3):
        shared = table_ref[j, pl.ds(step, 1), :]
        for layer in range(2):
            mod_ref[pl.ds(3 * layer + j, 1), :] = shared + shift_ref[j, pl.ds(layer, 1), :]
    tokens = jnp.concatenate([own_ref[...], pair_ref[...]], axis=0)
    normed = layer_norm(tokens, mod_ref[pl.ds(0, 1), :], mod_ref[pl.ds(1, 1), :])
    copies[0].wait()
    pieces = project(normed, qkv0_ref[...], gain_ref[0, 0], gain_ref[0, 1], heads)
    for i, piece in enumerate(pieces):
        packed_ref[i] = piece
    for copy in copies[1:]:
        copy.wait()


def pair_kernel(sizes, own_ref, pair_ref, gain_ref, qkv_ref, packed_ref):
    heads, layer = sizes
    tokens = jnp.concatenate([own_ref[...], pair_ref[...]], axis=0)
    pieces = project(tokens, qkv_ref[...], gain_ref[layer, 0], gain_ref[layer, 1], heads)
    for i, piece in enumerate(pieces):
        packed_ref[i] = piece


def block_kernel(sizes, *refs):
    heads, rows, layer, piece_rows, blocks = sizes
    others = refs[: blocks - 2]
    packed_ref, gain_ref, qkv_ref, out_ref = refs[blocks - 2 : blocks + 2]
    rest = refs[blocks + 2 :]
    tokens = jnp.concatenate([ref[...] for ref in others], axis=0)
    if layer == 0:
        mod_ref, send_ref, keep_ref = rest
        tokens = layer_norm(tokens, mod_ref[pl.ds(0, 1), :], mod_ref[pl.ds(1, 1), :])
    else:
        send_ref, keep_ref = rest
    pieces = project(tokens, qkv_ref[...], gain_ref[layer, 0], gain_ref[layer, 1], heads)
    everything = [jnp.concatenate([packed_ref[i], pieces[i]], axis=1) for i in range(3 * heads)]
    attended = []
    if layer == 0:
        for head in range(heads):
            attended.append(attend(*everything[3 * head : 3 * head + 3], None))
    else:
        width = 2 * rows
        key = lax.broadcasted_iota(jnp.int32, (width, width), 0)
        query = lax.broadcasted_iota(jnp.int32, (width, width), 1)
        same = (key // rows == query // rows) & (key % piece_rows == query % piece_rows)
        mask = same.astype(F32)
        for head in range(heads):
            parts = []
            for start in range(0, blocks * rows, width):
                cut = [value[:, start : start + width] for value in everything[3 * head : 3 * head + 3]]
                parts.append(attend(*cut, mask))
            attended.append(jnp.concatenate(parts, axis=1))
    stacked = jnp.concatenate(attended, axis=0).astype(BF16)
    partial = lax.dot_general(stacked, out_ref[...], (((0,), (0,)), ((), ())), preferred_element_type=F32)
    for i in range(blocks // 2):
        keep_ref[i * rows : (i + 1) * rows] = partial[2 * i * rows : (2 * i + 1) * rows]
        send_ref[i * rows : (i + 1) * rows] = partial[(2 * i + 1) * rows : (2 * i + 2) * rows].astype(BF16)


def fold_kernel(keep_ref, got_ref, send_ref, kept_ref):
    half = send_ref.shape[0]
    kept_ref[...] = keep_ref[:half] + got_ref[:half].astype(F32)
    send_ref[...] = (keep_ref[half:] + got_ref[half:].astype(F32)).astype(BF16)


def finish_kernel(pieces, keep_ref, got_ref, *piece_refs):
    update = (keep_ref[...] + got_ref[...].astype(F32)).astype(BF16)
    piece_rows = update.shape[0] // pieces
    for k in range(pieces):
        piece_refs[k][...] = update[k * piece_rows : (k + 1) * piece_rows]


def shuffle(values, place, piece_rows):
    count = values.shape[0]
    row = lax.broadcasted_iota(jnp.int32, (count, count), 0)
    column = lax.broadcasted_iota(jnp.int32, (count, count), 1)
    wanted = (place ^ (row // piece_rows)) * piece_rows + row % piece_rows
    return jnp.dot((wanted == column).astype(BF16), values, preferred_element_type=F32)


def middle_kernel(pieces, place_ref, own_ref, keep_ref, got_ref, mod_ref, current_ref, *piece_refs):
    update = keep_ref[...] + got_ref[...].astype(F32)
    current = (own_ref[...].astype(F32) + mod_ref[pl.ds(2, 1), :] * update).astype(BF16)
    current_ref[...] = current
    normed = layer_norm(current, mod_ref[pl.ds(3, 1), :], mod_ref[pl.ds(4, 1), :])
    piece_rows = normed.shape[0] // pieces
    ordered = shuffle(normed, place_ref[0], piece_rows).astype(BF16)
    for k in range(pieces):
        piece_refs[k][...] = ordered[k * piece_rows : (k + 1) * piece_rows]


def last_kernel(pieces, place_ref, current_ref, mod_ref, *refs):
    update = jnp.concatenate([ref[...] for ref in refs[:pieces]], axis=0)
    update = shuffle(update, place_ref[0], update.shape[0] // pieces)
    refs[pieces][0] = (current_ref[...].astype(F32) + mod_ref[pl.ds(5, 1), :] * update).astype(BF16)


def exchange(values, axis, count, flip):
    return lax.ppermute(values, axis, [(i, i ^ flip) for i in range(count)])


def body(head_count, sub_count, seq_count, latents, timestep, time_table, shift_table, qkv_weight, norm_gains, out_weight):
    rows, width = latents.shape[1:]
    heads, triple = qkv_weight.shape[2:]
    dim = triple // 3
    depth = out_weight.shape[1]
    blocks = head_count * sub_count
    piece_rows = rows // seq_count
    own = latents[0]
    shape = jax.ShapeDtypeStruct

    def spread(values):
        held = {0: values}
        flip = 1
        while flip < head_count:
            for j in list(held):
                held[j | 2 * flip] = exchange(held[j], "head", head_count, flip)
            flip *= 2
        return held, exchange(values, "sub", sub_count, 1)

    def relay(held, packed):
        far = [held[j] for j in sorted(held) if j]
        far, packed = lax.optimization_barrier((far, packed))
        return [v for value in far for v in (value, exchange(value, "sub", sub_count, 1))], packed

    def scatter(send, keep):
        got = exchange(send, "sub", sub_count, 1)
        flip = head_count // 2
        while flip:
            half = keep.shape[0] // 2
            send, keep = call(
                fold_kernel, "fold", (shape((half, width), BF16), shape((half, width), F32)), [VMEM] * 2, moved=half * width * 20
            )(keep, got)
            got = exchange(send, "head", head_count, flip)
            flip //= 2
        return keep, got

    qkv = qkv_weight.transpose(0, 2, 3, 1).reshape(2, heads * triple, width)
    gains = jnp.broadcast_to(norm_gains[..., None], norm_gains.shape + (1,))
    place = lax.axis_index("seq").astype(jnp.int32).reshape(1)

    held, pair = spread(own)
    packed_shape = shape((3 * heads, dim, 2 * rows), BF16)
    work = 2 * 2 * rows * heads * triple * width
    mods, packed, qkv0, qkv1, out0, out1 = call(
        functools.partial(first_kernel, (heads, rows, dim)),
        "first",
        (shape((8, width), F32), packed_shape, shape(qkv.shape[1:], BF16), shape(qkv.shape[1:], BF16),
         shape((depth, width), BF16), shape((depth, width), BF16)),
        [SMEM, VMEM, VMEM, VMEM, VMEM, VMEM, HBM, HBM],
        [pltpu.SemaphoreType.DMA((4,))],
        flops=work,
        moved=qkv.size * 2,
    )(timestep, time_table.transpose(1, 0, 2), shift_table.transpose(1, 0, 2), own, pair, gains, qkv, out_weight)

    half_rows = blocks // 2 * rows

    def block(layer, packed, others, qkv, out, extra):
        return call(
            functools.partial(block_kernel, (heads, rows, layer, piece_rows, blocks)),
            "block%d" % layer,
            (shape((half_rows, width), BF16), shape((half_rows, width), F32)),
            [VMEM] * (len(others) + 4 + len(extra)),
            flops=work * (blocks - 2) // 2 + 2 * blocks * rows * depth * width,
            moved=qkv.size * 2,
        )(*others, packed, gains, qkv, out, *extra)

    others, packed = relay(held, packed)
    send, keep = block(0, packed, others, qkv0, out0, [mods])
    keep, got = scatter(send, keep)
    current, *mine = call(
        functools.partial(middle_kernel, seq_count),
        "middle",
        (shape((rows, width), BF16),) + (shape((piece_rows, width), BF16),) * seq_count,
        [SMEM] + [VMEM] * 4,
        moved=rows * width * 8,
    )(place, own, keep, got, mods)
    theirs = [mine[0]] + [exchange(mine[k], "seq", seq_count, k) for k in range(1, seq_count)]
    mine = jnp.concatenate(theirs, axis=0)
    held, pair = spread(mine)
    packed = call(
        functools.partial(pair_kernel, (heads, 1)),
        "pair",
        packed_shape,
        [VMEM] * 4,
        flops=work,
        moved=qkv.size,
    )(mine, pair, gains, qkv1)
    others, packed = relay(held, packed)
    send, keep = block(1, packed, others, qkv1, out1, [])
    keep, got = scatter(send, keep)
    mine = call(
        functools.partial(finish_kernel, seq_count),
        "finish",
        (shape((piece_rows, width), BF16),) * seq_count,
        [VMEM] * 2,
        moved=rows * width * 8,
    )(keep, got)
    theirs = [mine[0]] + [exchange(mine[k], "seq", seq_count, k) for k in range(1, seq_count)]
    return call(
        functools.partial(last_kernel, seq_count),
        "last",
        shape((1, rows, width), BF16),
        [SMEM] + [VMEM] * (2 + seq_count),
        moved=rows * width * 8,
    )(place, current, mods, *theirs)


def solution(mesh):
    return jax.shard_map(
        functools.partial(body, mesh.shape["head"], mesh.shape["sub"], mesh.shape["seq"]),
        mesh=mesh,
        in_specs=(
            P(("grp", "seq"), ("head", "sub"), None),
            P("grp"),
            P(),
            P(),
            P(None, None, ("head", "sub"), None),
            P(),
            P(None, ("head", "sub"), None),
        ),
        out_specs=P(("grp", "seq"), ("head", "sub"), None),
        check_vma=False,
    )
```

```python
import functools

import jax
import jax.numpy as jnp
from jax import lax
from jax.experimental import pallas as pl
from jax.experimental.pallas import tpu as pltpu
from jax.sharding import PartitionSpec as P

EPSILON = 1e-06
F32 = jnp.float32
BF16 = jnp.bfloat16
VMEM = pl.BlockSpec(memory_space=pltpu.VMEM)
SMEM = pl.BlockSpec(memory_space=pltpu.SMEM)
HBM = pl.BlockSpec(memory_space=pltpu.HBM)


def call(kernel, name, out_shape, in_specs, scratch=(), flops=0, moved=0, limit=24):
    return pl.pallas_call(
        kernel,
        name=name,
        out_shape=out_shape,
        in_specs=in_specs,
        out_specs=jax.tree.map(lambda _: VMEM, out_shape, is_leaf=lambda leaf: hasattr(leaf, "dtype")),
        scratch_shapes=list(scratch),
        compiler_params=pltpu.CompilerParams(vmem_limit_bytes=limit * 1024 * 1024),
        cost_estimate=pl.CostEstimate(flops=flops, bytes_accessed=moved, transcendentals=0),
    )


def layer_norm(rows, shift_row, scale_row):
    wide = rows.astype(F32)
    center = jnp.mean(wide, axis=-1, keepdims=True)
    moved = wide - center
    spread = jnp.mean(moved * moved, axis=-1, keepdims=True)
    return (moved * lax.rsqrt(spread + EPSILON) * (1.0 + scale_row) + shift_row).astype(BF16)


def project(normed, weight, gain_q, gain_k, heads):
    flat = lax.dot_general(weight, normed, (((1,), (1,)), ((), ())), preferred_element_type=F32)
    dim = flat.shape[0] // (3 * heads)
    pieces = []
    for head in range(heads):
        for part, gain in ((0, gain_q), (1, gain_k), (2, None)):
            start = (3 * head + part) * dim
            values = flat[start : start + dim]
            if gain is not None:
                power = jnp.mean(values * values, axis=0, keepdims=True)
                values = values * lax.rsqrt(power + EPSILON) * gain
            pieces.append(values.astype(BF16))
    return pieces


def attend(queries, keys, values, mask):
    dim = queries.shape[0]
    scores = lax.dot_general(keys, queries, (((0,), (0,)), ((), ())), preferred_element_type=F32)
    weights = jnp.exp(scores * dim ** (-0.5))
    if mask is not None:
        weights = weights * mask
    total = jnp.sum(weights, axis=0, keepdims=True)
    mixed = jnp.dot(values, weights.astype(BF16), preferred_element_type=F32)
    return mixed / total


def first_kernel(sizes, step_ref, table_hbm, shift_hbm, own_hbm, pair_ref, gain_ref, qkv_hbm, out_hbm,
                 mod_ref, packed_ref, own_ref, qkv0_ref, qkv1_ref, out0_ref, out1_ref, table_ref, shift_ref, sems):
    heads, rows, dim = sizes
    copies = [
        pltpu.make_async_copy(source, target, sems.at[i])
        for i, (source, target) in enumerate(
            ((table_hbm, table_ref), (shift_hbm, shift_ref), (own_hbm, own_ref), (qkv_hbm.at[0], qkv0_ref),
             (out_hbm.at[0], out0_ref), (qkv_hbm.at[1], qkv1_ref), (out_hbm.at[1], out1_ref))
        )
    ]
    for copy in copies:
        copy.start()
    step = step_ref[0]
    for copy in copies[:3]:
        copy.wait()
    for j in range(3):
        shared = table_ref[j, pl.ds(step, 1), :]
        for layer in range(2):
            mod_ref[pl.ds(3 * layer + j, 1), :] = shared + shift_ref[j, pl.ds(layer, 1), :]
    tokens = jnp.concatenate([own_ref[...], pair_ref[...]], axis=0)
    normed = layer_norm(tokens, mod_ref[pl.ds(0, 1), :], mod_ref[pl.ds(1, 1), :])
    copies[3].wait()
    pieces = project(normed, qkv0_ref[...], gain_ref[0, 0], gain_ref[0, 1], heads)
    for i, piece in enumerate(pieces):
        packed_ref[i] = piece
    for copy in copies[4:]:
        copy.wait()


def pair_kernel(sizes, own_ref, pair_ref, gain_ref, qkv_ref, packed_ref):
    heads, layer = sizes
    tokens = jnp.concatenate([own_ref[...], pair_ref[...]], axis=0)
    pieces = project(tokens, qkv_ref[...], gain_ref[layer, 0], gain_ref[layer, 1], heads)
    for i, piece in enumerate(pieces):
        packed_ref[i] = piece


def block_kernel(sizes, *refs):
    heads, rows, layer, piece_rows, blocks = sizes
    others = refs[: blocks - 2]
    packed_ref, gain_ref, qkv_ref, out_ref = refs[blocks - 2 : blocks + 2]
    rest = refs[blocks + 2 :]
    tokens = jnp.concatenate([ref[...] for ref in others], axis=0)
    if layer == 0:
        mod_ref, send_ref, keep_ref = rest
        tokens = layer_norm(tokens, mod_ref[pl.ds(0, 1), :], mod_ref[pl.ds(1, 1), :])
    else:
        send_ref, keep_ref = rest
    pieces = project(tokens, qkv_ref[...], gain_ref[layer, 0], gain_ref[layer, 1], heads)
    everything = [jnp.concatenate([packed_ref[i], pieces[i]], axis=1) for i in range(3 * heads)]
    attended = []
    if layer == 0:
        for head in range(heads):
            attended.append(attend(*everything[3 * head : 3 * head + 3], None))
    else:
        width = 2 * rows
        key = lax.broadcasted_iota(jnp.int32, (width, width), 0)
        query = lax.broadcasted_iota(jnp.int32, (width, width), 1)
        same = (key // rows == query // rows) & (key % piece_rows == query % piece_rows)
        mask = same.astype(F32)
        for head in range(heads):
            parts = []
            for start in range(0, blocks * rows, width):
                cut = [value[:, start : start + width] for value in everything[3 * head : 3 * head + 3]]
                parts.append(attend(*cut, mask))
            attended.append(jnp.concatenate(parts, axis=1))
    stacked = jnp.concatenate(attended, axis=0).astype(BF16)
    partial = lax.dot_general(stacked, out_ref[...], (((0,), (0,)), ((), ())), preferred_element_type=F32)
    for i in range(blocks // 2):
        keep_ref[i * rows : (i + 1) * rows] = partial[2 * i * rows : (2 * i + 1) * rows]
        send_ref[i * rows : (i + 1) * rows] = partial[(2 * i + 1) * rows : (2 * i + 2) * rows].astype(BF16)


def fold_kernel(keep_ref, got_ref, send_ref, kept_ref):
    half = send_ref.shape[0]
    kept_ref[...] = keep_ref[:half] + got_ref[:half].astype(F32)
    send_ref[...] = (keep_ref[half:] + got_ref[half:].astype(F32)).astype(BF16)


def finish_kernel(pieces, keep_ref, got_ref, *piece_refs):
    update = (keep_ref[...] + got_ref[...].astype(F32)).astype(BF16)
    piece_rows = update.shape[0] // pieces
    for k in range(pieces):
        piece_refs[k][...] = update[k * piece_rows : (k + 1) * piece_rows]


def shuffle(values, place, piece_rows):
    count = values.shape[0]
    row = lax.broadcasted_iota(jnp.int32, (count, count), 0)
    column = lax.broadcasted_iota(jnp.int32, (count, count), 1)
    wanted = (place ^ (row // piece_rows)) * piece_rows + row % piece_rows
    return jnp.dot((wanted == column).astype(BF16), values, preferred_element_type=F32)


def middle_kernel(pieces, own_ref, keep_ref, got_ref, mod_ref, current_ref, *piece_refs):
    update = keep_ref[...] + got_ref[...].astype(F32)
    current = (own_ref[...].astype(F32) + mod_ref[pl.ds(2, 1), :] * update).astype(BF16)
    current_ref[...] = current
    normed = layer_norm(current, mod_ref[pl.ds(3, 1), :], mod_ref[pl.ds(4, 1), :])
    piece_rows = normed.shape[0] // pieces
    ordered = shuffle(normed, lax.axis_index("seq"), piece_rows).astype(BF16)
    for k in range(pieces):
        piece_refs[k][...] = ordered[k * piece_rows : (k + 1) * piece_rows]


def last_kernel(pieces, current_ref, mod_ref, *refs):
    update = jnp.concatenate([ref[...] for ref in refs[:pieces]], axis=0)
    update = shuffle(update, lax.axis_index("seq"), update.shape[0] // pieces)
    refs[pieces][0] = (current_ref[...].astype(F32) + mod_ref[pl.ds(5, 1), :] * update).astype(BF16)


def in_hbm(values):
    return pltpu.with_memory_space_constraint(values, pltpu.HBM)


def exchange(values, axis, count, flip):
    return lax.ppermute(values, axis, [(i, i ^ flip) for i in range(count)])


def body(head_count, sub_count, seq_count, latents, timestep, time_table, shift_table, qkv_weight, norm_gains, out_weight):
    rows, width = latents.shape[1:]
    heads, triple = qkv_weight.shape[2:]
    dim = triple // 3
    depth = out_weight.shape[1]
    blocks = head_count * sub_count
    piece_rows = rows // seq_count
    own = latents[0]
    shape = pltpu.VMEM

    def spread(values):
        held = {0: values}
        flip = 1
        while flip < head_count:
            for j in list(held):
                held[j | 2 * flip] = exchange(held[j], "head", head_count, flip)
            flip *= 2
        return held, exchange(values, "sub", sub_count, 1)

    def relay(held, packed):
        far = [held[j] for j in sorted(held) if j]
        far, packed = lax.optimization_barrier((far, packed))
        return [v for value in far for v in (value, exchange(value, "sub", sub_count, 1))], packed

    def scatter(send, keep):
        got = exchange(send, "sub", sub_count, 1)
        flip = head_count // 2
        while flip:
            half = keep.shape[0] // 2
            send, keep = call(
                fold_kernel, "fold", (shape((half, width), BF16), shape((half, width), F32)), [VMEM] * 2, moved=half * width * 20
            )(keep, got)
            got = exchange(send, "head", head_count, flip)
            flip //= 2
        return keep, got

    qkv = qkv_weight.transpose(0, 2, 3, 1).reshape(2, heads * triple, width)
    gains = jnp.broadcast_to(norm_gains[..., None], norm_gains.shape + (1,))

    held, pair = spread(own)
    packed_shape = shape((3 * heads, dim, 2 * rows), BF16)
    work = 2 * 2 * rows * heads * triple * width
    table = time_table.transpose(1, 0, 2)
    shift = shift_table.transpose(1, 0, 2)
    mods, packed, mine, qkv0, qkv1, out0, out1 = call(
        functools.partial(first_kernel, (heads, rows, dim)),
        "first",
        (shape((8, width), F32), packed_shape, shape((rows, width), BF16), shape(qkv.shape[1:], BF16), shape(qkv.shape[1:], BF16),
         shape((depth, width), BF16), shape((depth, width), BF16)),
        [SMEM, HBM, HBM, HBM, VMEM, VMEM, HBM, HBM],
        [pltpu.VMEM(table.shape, F32), pltpu.VMEM(shift.shape, F32), pltpu.SemaphoreType.DMA((7,))],
        flops=work,
        moved=qkv.size * 2,
    )(timestep, in_hbm(table), in_hbm(shift), in_hbm(own), pair, gains, in_hbm(qkv), in_hbm(out_weight))

    half_rows = blocks // 2 * rows

    def block(layer, packed, others, qkv, out, extra):
        return call(
            functools.partial(block_kernel, (heads, rows, layer, piece_rows, blocks)),
            "block%d" % layer,
            (shape((half_rows, width), BF16), shape((half_rows, width), F32)),
            [VMEM] * (len(others) + 4 + len(extra)),
            flops=work * (blocks - 2) // 2 + 2 * blocks * rows * depth * width,
            moved=qkv.size * 2,
        )(*others, packed, gains, qkv, out, *extra)

    others, packed = relay(held, packed)
    send, keep = block(0, packed, others, qkv0, out0, [mods])
    keep, got = scatter(send, keep)
    current, *mine = call(
        functools.partial(middle_kernel, seq_count),
        "middle",
        (shape((rows, width), BF16),) + (shape((piece_rows, width), BF16),) * seq_count,
        [VMEM] * 4,
        moved=rows * width * 8,
    )(mine, keep, got, mods)
    theirs = [mine[0]] + [exchange(mine[k], "seq", seq_count, k) for k in range(1, seq_count)]
    mine = jnp.concatenate(theirs, axis=0)
    held, pair = spread(mine)
    packed = call(
        functools.partial(pair_kernel, (heads, 1)),
        "pair",
        packed_shape,
        [VMEM] * 4,
        flops=work,
        moved=qkv.size,
    )(mine, pair, gains, qkv1)
    others, packed = relay(held, packed)
    send, keep = block(1, packed, others, qkv1, out1, [])
    keep, got = scatter(send, keep)
    mine = call(
        functools.partial(finish_kernel, seq_count),
        "finish",
        (shape((piece_rows, width), BF16),) * seq_count,
        [VMEM] * 2,
        moved=rows * width * 8,
    )(keep, got)
    theirs = [mine[0]] + [exchange(mine[k], "seq", seq_count, k) for k in range(1, seq_count)]
    return call(
        functools.partial(last_kernel, seq_count),
        "last",
        jax.ShapeDtypeStruct((1, rows, width), BF16),
        [VMEM] * (2 + seq_count),
        moved=rows * width * 8,
    )(current, mods, *theirs)


def solution(mesh):
    return jax.shard_map(
        functools.partial(body, mesh.shape["head"], mesh.shape["sub"], mesh.shape["seq"]),
        mesh=mesh,
        in_specs=(
            P(("grp", "seq"), ("head", "sub"), None),
            P("grp"),
            P(),
            P(),
            P(None, None, ("head", "sub"), None),
            P(),
            P(None, ("head", "sub"), None),
        ),
        out_specs=P(("grp", "seq"), ("head", "sub"), None),
        check_vma=False,
    )
```

```python
import functools

import jax
import jax.numpy as jnp
from jax import lax
from jax.experimental import pallas as pl
from jax.experimental.pallas import tpu as pltpu
from jax.sharding import PartitionSpec as P

EPSILON = 1e-06
F32 = jnp.float32
BF16 = jnp.bfloat16
VMEM = pl.BlockSpec(memory_space=pltpu.VMEM)
SMEM = pl.BlockSpec(memory_space=pltpu.SMEM)
HBM = pl.BlockSpec(memory_space=pltpu.HBM)


def call(kernel, out_shape, in_specs, scratch=(), flops=0, moved=0):
    return pl.pallas_call(
        kernel,
        out_shape=out_shape,
        in_specs=in_specs,
        out_specs=jax.tree.map(lambda _: VMEM, out_shape, is_leaf=lambda leaf: hasattr(leaf, "dtype")),
        scratch_shapes=list(scratch),
        compiler_params=pltpu.CompilerParams(vmem_limit_bytes=24 * 1024 * 1024),
        cost_estimate=pl.CostEstimate(flops=flops, bytes_accessed=moved, transcendentals=0),
    )


def in_hbm(values):
    return pltpu.with_memory_space_constraint(values, pltpu.HBM)


def layer_norm(rows, shift_row, scale_row):
    wide = rows.astype(F32)
    center = jnp.mean(wide, axis=-1, keepdims=True)
    moved = wide - center
    spread = jnp.mean(moved * moved, axis=-1, keepdims=True)
    return (moved * lax.rsqrt(spread + EPSILON) * (1.0 + scale_row) + shift_row).astype(BF16)


def shuffle(values, rows, piece_rows):
    place = lax.axis_index("seq")
    count = values.shape[0]
    row = lax.broadcasted_iota(jnp.int32, (count, count), 0)
    column = lax.broadcasted_iota(jnp.int32, (count, count), 1)
    inside = row % rows
    wanted = row - inside + (place ^ (inside // piece_rows)) * piece_rows + inside % piece_rows
    return jnp.dot((wanted == column).astype(BF16), values, preferred_element_type=F32).astype(BF16)


def project(normed, weight, gain_ref, layer, heads):
    flat = lax.dot_general(weight, normed, (((1,), (1,)), ((), ())), preferred_element_type=F32)
    dim = flat.shape[0] // (3 * heads)
    pieces = []
    for head in range(heads):
        for part in range(3):
            start = (3 * head + part) * dim
            values = flat[start : start + dim]
            if part < 2:
                power = jnp.mean(values * values, axis=0, keepdims=True)
                values = values * lax.rsqrt(power + EPSILON) * gain_ref[2 * layer + part]
            pieces.append(values.astype(BF16))
    return pieces


def attend(queries, keys, values, mask):
    dim = queries.shape[0]
    scores = lax.dot_general(keys, queries, (((0,), (0,)), ((), ())), preferred_element_type=F32)
    weights = jnp.exp(scores * dim ** (-0.5))
    if mask is not None:
        weights = weights * mask
    total = jnp.sum(weights, axis=0, keepdims=True)
    mixed = jnp.dot(values, weights.astype(BF16), preferred_element_type=F32)
    return mixed / total


def first_kernel(sizes, step_ref, table_hbm, shift_hbm, own_hbm, pair_ref, norm_hbm, qkv_hbm, out_hbm,
                 mod_ref, gain_ref, packed_ref, own_ref, qkv0_ref, qkv1_ref, out0_ref, out1_ref,
                 table_ref, shift_ref, norm_ref, raw_ref, sems):
    heads, rows, piece_rows, dim = sizes
    copies = [
        pltpu.make_async_copy(source, target, sems.at[i])
        for i, (source, target) in enumerate(
            ((table_hbm, table_ref), (shift_hbm, shift_ref), (norm_hbm, norm_ref),
             (own_hbm, raw_ref), (qkv_hbm.at[0], qkv0_ref),
             (out_hbm.at[0], out0_ref), (qkv_hbm.at[1], qkv1_ref), (out_hbm.at[1], out1_ref))
        )
    ]
    for copy in copies:
        copy.start()
    for copy in copies[:4]:
        copy.wait()
    step = step_ref[0]
    for j in range(3):
        shared = table_ref[j, pl.ds(step, 1), :]
        for layer in range(2):
            mod_ref[pl.ds(3 * layer + j, 1), :] = shared + shift_ref[j, pl.ds(layer, 1), :]
    diagonal = lax.broadcasted_iota(jnp.int32, (dim, dim), 0) == lax.broadcasted_iota(jnp.int32, (dim, dim), 1)
    for layer in range(2):
        for part in range(2):
            spread = jnp.where(diagonal, norm_ref[layer, pl.ds(part, 1), :], 0.0)
            gain_ref[2 * layer + part] = jnp.sum(spread, axis=1, keepdims=True)
    own_ref[...] = shuffle(raw_ref[...], rows, piece_rows)
    tokens = jnp.concatenate([raw_ref[...], pair_ref[...]], axis=0)
    normed = layer_norm(tokens, mod_ref[pl.ds(0, 1), :], mod_ref[pl.ds(1, 1), :])
    normed = shuffle(normed, rows, piece_rows)
    copies[4].wait()
    for i, piece in enumerate(project(normed, qkv0_ref[...], gain_ref, 0, heads)):
        packed_ref[i] = piece
    for copy in copies[5:]:
        copy.wait()


def pair_kernel(heads, token_ref, gain_ref, qkv_ref, packed_ref):
    for i, piece in enumerate(project(token_ref[...], qkv_ref[...], gain_ref, 1, heads)):
        packed_ref[i] = piece


def block_kernel(sizes, *refs):
    heads, rows, piece_rows, sets, others, layer = sizes
    far = refs[:others]
    packed_ref, gain_ref, qkv_ref, out_ref = refs[others : others + 4]
    rest = refs[others + 4 :]
    tokens = jnp.concatenate([ref[...] for ref in far], axis=0) if others > 1 else far[0][...]
    if layer == 0:
        mod_ref, send_ref, keep_ref, theirs_ref = rest
        theirs_ref[...] = shuffle(far[0][...], rows, piece_rows)
        tokens = layer_norm(tokens, mod_ref[pl.ds(0, 1), :], mod_ref[pl.ds(1, 1), :])
        tokens = shuffle(tokens, rows, piece_rows)
    else:
        send_ref, keep_ref = rest
    pieces = project(tokens, qkv_ref[...], gain_ref, layer, heads)
    everything = [jnp.concatenate([packed_ref[i], pieces[i]], axis=1) for i in range(3 * heads)]
    attended = []
    if layer == 0:
        for head in range(heads):
            attended.append(attend(*everything[3 * head : 3 * head + 3], None))
    else:
        key = lax.broadcasted_iota(jnp.int32, (rows, rows), 0)
        query = lax.broadcasted_iota(jnp.int32, (rows, rows), 1)
        mask = (key % piece_rows == query % piece_rows).astype(F32)
        for head in range(heads):
            parts = []
            for start in range(0, sets * rows, rows):
                cut = [value[:, start : start + rows] for value in everything[3 * head : 3 * head + 3]]
                parts.append(attend(*cut, mask))
            attended.append(jnp.concatenate(parts, axis=1))
    stacked = jnp.concatenate(attended, axis=0).astype(BF16)
    partial = lax.dot_general(stacked, out_ref[...], (((0,), (0,)), ((), ())), preferred_element_type=F32)
    for i in range(sets // 2):
        keep_ref[i * rows : (i + 1) * rows] = partial[2 * i * rows : (2 * i + 1) * rows]
        send_ref[i * rows : (i + 1) * rows] = partial[(2 * i + 1) * rows : (2 * i + 2) * rows].astype(BF16)


def fold_kernel(keep_ref, got_ref, send_ref, kept_ref):
    half = send_ref.shape[0]
    kept_ref[...] = keep_ref[:half] + got_ref[:half].astype(F32)
    send_ref[...] = (keep_ref[half:] + got_ref[half:].astype(F32)).astype(BF16)


def split_kernel(keep_ref, got_ref, near_ref, far_ref, kept_ref):
    total = keep_ref[...] + got_ref[...].astype(F32)
    kept_ref[...] = total
    rows = total.shape[0] // 2
    half = rows // 2
    sent = total.astype(BF16)
    near_ref[...] = jnp.concatenate([sent[rows : rows + half], sent[:half]], axis=0)
    far_ref[...] = jnp.concatenate([sent[rows + half :], sent[half:rows]], axis=0)


def middle_kernel(start, piece_rows, kept_ref, got_ref, own_ref, theirs_ref, mod_ref, *refs):
    current_ref, *piece_refs = refs[-1 - own_ref.shape[0] // 2 // piece_rows :]
    rows = own_ref.shape[0]
    half = rows // 2
    total = jnp.concatenate([kept_ref[start : start + half], kept_ref[rows + start : rows + start + half]], axis=0)
    before = jnp.concatenate([own_ref[start : start + half], theirs_ref[start : start + half]], axis=0)
    update = total + got_ref[...].astype(F32)
    current = (before.astype(F32) + mod_ref[pl.ds(2, 1), :] * update).astype(BF16)
    current_ref[...] = current[:half]
    normed = layer_norm(current, mod_ref[pl.ds(3, 1), :], mod_ref[pl.ds(4, 1), :])
    for k, ref in enumerate(piece_refs):
        at = k * piece_rows
        ref[:piece_rows] = normed[at : at + piece_rows]
        ref[piece_rows:] = normed[half + at : half + at + piece_rows]


def merge_kernel(pieces, keep_ref, got_ref, send_ref, kept_ref):
    total = keep_ref[...] + got_ref[...].astype(F32)
    width = total.shape[0] // pieces
    half = width // 2
    for k in range(pieces):
        kept_ref[k * half : (k + 1) * half] = total[k * width : k * width + half]
        send_ref[k * half : (k + 1) * half] = total[k * width + half : (k + 1) * width].astype(BF16)


def finish_kernel(pieces, keep_ref, got_ref, *piece_refs):
    update = (keep_ref[...] + got_ref[...].astype(F32)).astype(BF16)
    piece_rows = update.shape[0] // pieces
    for k in range(pieces):
        piece_refs[k][...] = update[k * piece_rows : (k + 1) * piece_rows]


def last_kernel(pieces, near_ref, far_ref, mod_ref, *refs):
    update = jnp.concatenate([ref[...] for ref in refs[:pieces]], axis=0).astype(F32)
    current = jnp.concatenate([near_ref[...], far_ref[...]], axis=0).astype(F32)
    mixed = (current + mod_ref[pl.ds(5, 1), :] * update).astype(BF16)
    refs[pieces][0] = shuffle(mixed, mixed.shape[0], mixed.shape[0] // pieces)


def exchange(values, axis, count, flip):
    return lax.ppermute(values, axis, [(i, i ^ flip) for i in range(count)])


def body(head_count, sub_count, seq_count, latents, timestep, time_table, shift_table, qkv_weight, norm_gains, out_weight):
    rows, width = latents.shape[1:]
    heads, triple = qkv_weight.shape[2:]
    dim = triple // 3
    depth = out_weight.shape[1]
    blocks = head_count * sub_count
    piece_rows = rows // seq_count
    own = latents[0]
    shape = pltpu.VMEM
    flips = [1 << bit for bit in range(head_count.bit_length() - 1)]

    def spread(values, flips):
        held = {0: values}
        for place, flip in enumerate(flips):
            for j in list(held):
                held[j | 2 << place] = exchange(held[j], "head", head_count, flip)
        return held

    def reduce(send, keep, flips):
        got = exchange(send, "sub", sub_count, 1)
        for flip in reversed(flips):
            half = keep.shape[0] // 2
            send, keep = call(
                fold_kernel, (shape((half, width), BF16), shape((half, width), F32)), [VMEM] * 2, moved=half * width * 20
            )(keep, got)
            got = exchange(send, "head", head_count, flip)
        return keep, got

    def block(layer, packed, others, qkv, out, extra):
        size = others[0].shape[0]
        sets = blocks * rows // size
        half = blocks // 2 * rows
        outputs = (shape((half, width), BF16), shape((half, width), F32))
        if layer == 0:
            outputs += (shape((rows, width), BF16),)
        return call(
            functools.partial(block_kernel, (heads, size, 2 * piece_rows if layer else piece_rows, sets, len(others), layer)),
            outputs,
            [VMEM] * (len(others) + 4 + len(extra)),
            flops=2 * len(others) * size * heads * triple * width + 2 * blocks * rows * depth * width,
            moved=qkv.size * 2,
        )(*others, packed, gains, qkv, out, *extra)

    qkv = qkv_weight.transpose(0, 2, 3, 1).reshape(2, heads * triple, width)
    table = time_table.transpose(1, 0, 2)
    shift = shift_table.transpose(1, 0, 2)
    packed_shape = shape((3 * heads, dim, 2 * rows), BF16)
    work = 2 * 2 * rows * heads * triple * width

    held = spread(own, flips)
    pair = exchange(own, "sub", sub_count, 1)
    mods, gains, packed, mine, qkv0, qkv1, out0, out1 = call(
        functools.partial(first_kernel, (heads, rows, piece_rows, dim)),
        (shape((8, width), F32), shape((4, dim, 1), F32), packed_shape, shape((rows, width), BF16),
         shape(qkv.shape[1:], BF16), shape(qkv.shape[1:], BF16), shape((depth, width), BF16), shape((depth, width), BF16)),
        [SMEM, HBM, HBM, HBM, VMEM, HBM, HBM, HBM],
        [pltpu.VMEM(table.shape, F32), pltpu.VMEM(shift.shape, F32),
         pltpu.VMEM(norm_gains.shape, F32), pltpu.VMEM(own.shape, BF16), pltpu.SemaphoreType.DMA((8,))],
        flops=work,
        moved=qkv.size * 2,
    )(timestep, in_hbm(table), in_hbm(shift), in_hbm(own), pair, in_hbm(norm_gains), in_hbm(qkv), in_hbm(out_weight))

    far = [held[j] for j in sorted(held) if j]
    far, packed = lax.optimization_barrier((far, packed))
    others = [v for value in far for v in (value, exchange(value, "sub", sub_count, 1))]
    send, keep, theirs = block(0, packed, others, qkv0, out0, [mods])

    keep, got = reduce(send, keep, flips[1:])
    near, distant, kept = call(
        split_kernel,
        (shape((rows, width), BF16), shape((rows, width), BF16), shape((2 * rows, width), F32)),
        [VMEM] * 2,
        moved=rows * width * 20,
    )(keep, got)
    distant = exchange(distant, "head", head_count, 1)
    near = exchange(near, "head", head_count, 1)
    middle = seq_count // 2

    def half_block(start, got, *after):
        return call(
            functools.partial(middle_kernel, start, piece_rows),
            (shape((rows // 2, width), BF16),) + (shape((2 * piece_rows, width), BF16),) * middle,
            [VMEM] * (5 + len(after)),
            moved=rows * width * 16,
        )(kept, got, mine, theirs, mods, *after)

    current_far, *pieces_far = half_block(rows // 2, distant)
    moved = {k: exchange(pieces_far[k - middle], "seq", seq_count, k) for k in reversed(range(middle, seq_count))}
    current_near, *pieces_near = half_block(0, near, current_far)
    moved.update({k: exchange(pieces_near[k], "seq", seq_count, k) for k in reversed(range(1, middle))})
    moved[0] = pieces_near[0]
    tokens = jnp.concatenate([moved[k] for k in range(seq_count)], axis=0)

    held = spread(tokens, flips[1:])
    for j in list(held):
        held[j | 1] = exchange(held[j], "sub", sub_count, 1)
    packed = call(
        functools.partial(pair_kernel, heads), packed_shape, [VMEM] * 3, flops=work, moved=qkv.size
    )(tokens, gains, qkv1)
    send, keep = block(1, packed, [held[j] for j in sorted(held) if j], qkv1, out1, [])

    keep, got = reduce(send, keep, flips[1:])
    send, keep = call(
        functools.partial(merge_kernel, seq_count),
        (shape((rows, width), BF16), shape((rows, width), F32)),
        [VMEM] * 2,
        moved=rows * width * 20,
    )(keep, got)
    got = exchange(send, "head", head_count, 1)
    pieces = call(
        functools.partial(finish_kernel, seq_count),
        (shape((piece_rows, width), BF16),) * seq_count,
        [VMEM] * 2,
        moved=rows * width * 8,
    )(keep, got)
    back = {k: exchange(pieces[k], "seq", seq_count, k) for k in reversed(range(1, seq_count))}
    back[0] = pieces[0]
    return call(
        functools.partial(last_kernel, seq_count),
        jax.ShapeDtypeStruct((1, rows, width), BF16),
        [VMEM] * (3 + seq_count),
        moved=rows * width * 8,
    )(current_near, current_far, mods, *[back[k] for k in range(seq_count)])


def solution(mesh):
    seq_count = mesh.shape["seq"]

    def named(*args):
        return body(mesh.shape["head"], mesh.shape["sub"], seq_count, *args)

    return jax.shard_map(
        named,
        mesh=mesh,
        in_specs=(
            P(("grp", "seq"), ("head", "sub"), None),
            P("grp"),
            P(),
            P(),
            P(None, None, ("head", "sub"), None),
            P(),
            P(None, ("head", "sub"), None),
        ),
        out_specs=P(("grp", "seq"), ("head", "sub"), None),
        check_vma=False,
    )
```

```python
import functools

import jax
import jax.numpy as jnp
from jax import lax
from jax.experimental import pallas as pl
from jax.experimental.pallas import tpu as pltpu
from jax.sharding import PartitionSpec as P

EPSILON = 1e-06
LOG2_E = 1.4426950408889634
F32 = jnp.float32
BF16 = jnp.bfloat16
VMEM = pl.BlockSpec(memory_space=pltpu.VMEM)
SMEM = pl.BlockSpec(memory_space=pltpu.SMEM)
HBM = pl.BlockSpec(memory_space=pltpu.HBM)


def call(kernel, out_shape, in_specs, scratch=(), flops=0, moved=0):
    return pl.pallas_call(
        kernel,
        out_shape=out_shape,
        in_specs=in_specs,
        out_specs=jax.tree.map(lambda _: VMEM, out_shape, is_leaf=lambda leaf: hasattr(leaf, "dtype")),
        scratch_shapes=list(scratch),
        compiler_params=pltpu.CompilerParams(vmem_limit_bytes=24 * 1024 * 1024),
        cost_estimate=pl.CostEstimate(flops=flops, bytes_accessed=moved, transcendentals=0),
    )


def in_hbm(values):
    return pltpu.with_memory_space_constraint(values, pltpu.HBM)


def layer_norm(rows, shift_row, scale_row):
    wide = rows.astype(F32)
    center = jnp.mean(wide, axis=-1, keepdims=True)
    moved = wide - center
    spread = jnp.mean(moved * moved, axis=-1, keepdims=True)
    return (moved * lax.rsqrt(spread + EPSILON) * (1.0 + scale_row) + shift_row).astype(BF16)


def shuffled(ref, piece_rows):
    place = lax.axis_index("seq")
    rows = ref.shape[0]
    if piece_rows % 16 == 0:
        starts = [pl.multiple_of((place ^ k) * piece_rows, piece_rows) for k in range(rows // piece_rows)]
        return jnp.concatenate([ref[pl.ds(start, piece_rows), :] for start in starts], axis=0)
    row = lax.broadcasted_iota(jnp.int32, (rows, rows), 0)
    column = lax.broadcasted_iota(jnp.int32, (rows, rows), 1)
    wanted = (place ^ (row // piece_rows)) * piece_rows + row % piece_rows
    return jnp.dot((wanted == column).astype(BF16), ref[...], preferred_element_type=F32).astype(BF16)


def project(normed, weight, gain_ref, layer, heads):
    flat = lax.dot_general(weight, normed, (((1,), (1,)), ((), ())), preferred_element_type=F32)
    dim = flat.shape[0] // (3 * heads)
    pieces = []
    for head in range(heads):
        for part in range(3):
            start = (3 * head + part) * dim
            values = flat[start : start + dim]
            if part < 2:
                power = jnp.mean(values * values, axis=0, keepdims=True)
                values = values * lax.rsqrt(power + EPSILON) * gain_ref[2 * layer + part]
            pieces.append(values.astype(BF16))
    return pieces


def attend(queries, keys, values, mask):
    scale = queries[0].shape[0] ** (-0.5) * LOG2_E
    scores = [lax.dot_general(k, q, (((0,), (0,)), ((), ())), preferred_element_type=F32) for q, k in zip(queries, keys)]
    weights = [jnp.exp2(score * scale) for score in scores]
    if mask is not None:
        weights = [weight * mask for weight in weights]
    totals = [jnp.sum(weight, axis=0, keepdims=True) for weight in weights]
    mixed = [jnp.dot(v, weight.astype(BF16), preferred_element_type=F32) for v, weight in zip(values, weights)]
    return [value * (1.0 / total) for value, total in zip(mixed, totals)]


def first_kernel(piece_rows, step_ref, table_hbm, shift_hbm, own_hbm, norm_hbm, qkv_hbm, out_hbm,
                 mod_ref, gain_ref, normed_ref, own_ref, qkv0_ref, qkv1_ref, out0_ref, out1_ref,
                 table_ref, shift_ref, norm_ref, raw_ref, sems):
    copies = [
        pltpu.make_async_copy(source, target, sems.at[i])
        for i, (source, target) in enumerate(
            ((table_hbm, table_ref), (shift_hbm, shift_ref), (norm_hbm, norm_ref), (own_hbm, raw_ref),
             (qkv_hbm.at[0], qkv0_ref), (out_hbm.at[0], out0_ref), (qkv_hbm.at[1], qkv1_ref), (out_hbm.at[1], out1_ref))
        )
    ]
    for copy in copies:
        copy.start()
    for copy in copies[:4]:
        copy.wait()
    step = step_ref[0]
    for j in range(3):
        shared = table_ref[j, pl.ds(step, 1), :]
        for layer in range(2):
            mod_ref[pl.ds(3 * layer + j, 1), :] = shared + shift_ref[j, pl.ds(layer, 1), :]
    dim = norm_ref.shape[2]
    diagonal = lax.broadcasted_iota(jnp.int32, (dim, dim), 0) == lax.broadcasted_iota(jnp.int32, (dim, dim), 1)
    for layer in range(2):
        for part in range(2):
            spread = jnp.where(diagonal, norm_ref[layer, pl.ds(part, 1), :], 0.0)
            gain_ref[2 * layer + part] = jnp.sum(spread, axis=1, keepdims=True)
    tokens = shuffled(raw_ref, piece_rows)
    own_ref[...] = tokens
    normed_ref[...] = layer_norm(tokens, mod_ref[pl.ds(0, 1), :], mod_ref[pl.ds(1, 1), :])
    for copy in copies[4:]:
        copy.wait()


def prepare_kernel(piece_rows, far, mod_ref, *refs):
    theirs_ref, normed_ref = refs[far:]
    tokens = [shuffled(ref, piece_rows) for ref in refs[:far]]
    theirs_ref[...] = tokens[1]
    tokens = jnp.concatenate(tokens, axis=0)
    normed_ref[...] = layer_norm(tokens, mod_ref[pl.ds(0, 1), :], mod_ref[pl.ds(1, 1), :])


def region(number):
    return pl.when(lax.axis_index("seq") >= -number)


def block_kernel(sizes, *refs):
    heads, rows, piece_rows, layer, raw, ready = sizes
    inputs = refs[: raw + ready]
    gain_ref, qkv_ref, out_ref = refs[raw + ready : raw + ready + 3]
    mod_ref = refs[raw + ready + 3]
    send_ref, keep_ref, token_ref, packed_ref, stack_ref = refs[-5:]
    sets = token_ref.shape[0] // rows

    if layer == 0:
        own_ref, near_ref = inputs[raw:]
        token_ref[:rows] = own_ref[...]
        for i in range(raw + 1):
            token_ref[max(1, 2 * i) * rows : (max(1, 2 * i) + 1) * rows] = near_ref[i * rows : (i + 1) * rows]
        for i in range(raw):
            fresh = shuffled(inputs[i], piece_rows)
            fresh = layer_norm(fresh, mod_ref[pl.ds(0, 1), :], mod_ref[pl.ds(1, 1), :])
            token_ref[(2 * i + 3) * rows : (2 * i + 4) * rows] = fresh
    else:
        for i, ref in enumerate(inputs):
            token_ref[i * rows : (i + 1) * rows] = ref[...]

    @region(1)
    def _():
        for i, piece in enumerate(project(token_ref[...], qkv_ref[...], gain_ref, layer, heads)):
            packed_ref[i] = piece

    @region(2)
    def _():
        dim = packed_ref.shape[1]
        span = token_ref.shape[0] if layer == 0 else rows
        mask = None
        if layer:
            key = lax.broadcasted_iota(jnp.int32, (rows, rows), 0)
            query = lax.broadcasted_iota(jnp.int32, (rows, rows), 1)
            mask = (key % piece_rows == query % piece_rows).astype(F32)
        places = [(head, start) for start in range(0, token_ref.shape[0], span) for head in range(heads)]
        cut = [[packed_ref[3 * head + part, :, start : start + span] for head, start in places] for part in range(3)]
        for (head, start), value in zip(places, attend(*cut, mask)):
            stack_ref[head * dim : (head + 1) * dim, start : start + span] = value.astype(BF16)

    @region(3)
    def _():
        partial = lax.dot_general(stack_ref[...], out_ref[...], (((0,), (0,)), ((), ())), preferred_element_type=F32)
        for i in range(sets // 2):
            keep_ref[i * rows : (i + 1) * rows] = partial[2 * i * rows : (2 * i + 1) * rows]
            send_ref[i * rows : (i + 1) * rows] = partial[(2 * i + 1) * rows : (2 * i + 2) * rows].astype(BF16)


def fold_kernel(keep_ref, got_ref, send_ref, kept_ref):
    half = send_ref.shape[0]
    kept_ref[...] = keep_ref[:half] + got_ref[:half].astype(F32)
    send_ref[...] = (keep_ref[half:] + got_ref[half:].astype(F32)).astype(BF16)


def split_kernel(keep_ref, got_ref, near_ref, far_ref, kept_ref):
    total = keep_ref[...] + got_ref[...].astype(F32)
    kept_ref[...] = total
    rows = total.shape[0] // 2
    half = rows // 2
    sent = total.astype(BF16)
    near_ref[...] = jnp.concatenate([sent[rows : rows + half], sent[:half]], axis=0)
    far_ref[...] = jnp.concatenate([sent[rows + half :], sent[half:rows]], axis=0)


def middle_kernel(start, piece_rows, kept_ref, got_ref, own_ref, theirs_ref, mod_ref, *refs):
    current_ref, *piece_refs = refs[-1 - own_ref.shape[0] // 2 // piece_rows :]
    rows = own_ref.shape[0]
    half = rows // 2
    total = jnp.concatenate([kept_ref[start : start + half], kept_ref[rows + start : rows + start + half]], axis=0)
    before = jnp.concatenate([own_ref[start : start + half], theirs_ref[start : start + half]], axis=0)
    update = total + got_ref[...].astype(F32)
    current = (before.astype(F32) + mod_ref[pl.ds(2, 1), :] * update).astype(BF16)
    current_ref[...] = current[:half]
    normed = layer_norm(current, mod_ref[pl.ds(3, 1), :], mod_ref[pl.ds(4, 1), :])
    for k, ref in enumerate(piece_refs):
        at = k * piece_rows
        ref[:piece_rows] = normed[at : at + piece_rows]
        ref[piece_rows:] = normed[half + at : half + at + piece_rows]


def merge_kernel(pieces, keep_ref, got_ref, send_ref, kept_ref):
    total = keep_ref[...] + got_ref[...].astype(F32)
    width = total.shape[0] // pieces
    half = width // 2
    for k in range(pieces):
        kept_ref[k * half : (k + 1) * half] = total[k * width : k * width + half]
        send_ref[k * half : (k + 1) * half] = total[k * width + half : (k + 1) * width].astype(BF16)


def finish_kernel(pieces, keep_ref, got_ref, *piece_refs):
    update = (keep_ref[...] + got_ref[...].astype(F32)).astype(BF16)
    piece_rows = update.shape[0] // pieces
    for k in range(pieces):
        piece_refs[k][...] = update[k * piece_rows : (k + 1) * piece_rows]


def last_kernel(pieces, near_ref, far_ref, mod_ref, *refs):
    update = jnp.concatenate([ref[...] for ref in refs[:pieces]], axis=0).astype(F32)
    current = jnp.concatenate([near_ref[...], far_ref[...]], axis=0).astype(F32)
    mixed = (current + mod_ref[pl.ds(5, 1), :] * update).astype(BF16)
    out_ref, mixed_ref = refs[pieces:]
    mixed_ref[...] = mixed
    out_ref[0] = shuffled(mixed_ref, mixed.shape[0] // pieces)


def exchange(values, axis, count, flip):
    return lax.ppermute(values, axis, [(i, i ^ flip) for i in range(count)])


def body(head_count, sub_count, seq_count, latents, timestep, time_table, shift_table, qkv_weight, norm_gains, out_weight):
    rows, width = latents.shape[1:]
    heads, triple = qkv_weight.shape[2:]
    dim = triple // 3
    depth = out_weight.shape[1]
    blocks = head_count * sub_count
    piece_rows = rows // seq_count
    own = latents[0]
    shape = pltpu.VMEM
    flips = [1 << bit for bit in range(head_count.bit_length() - 1)]

    def spread(values, flips):
        held = {0: values}
        for place, flip in enumerate(flips):
            for j in list(held):
                held[j | 2 << place] = exchange(held[j], "head", head_count, flip)
        return held

    def reduce(send, keep, flips):
        got = exchange(send, "sub", sub_count, 1)
        for flip in reversed(flips):
            half = keep.shape[0] // 2
            send, keep = call(
                fold_kernel, (shape((half, width), BF16), shape((half, width), F32)), [VMEM] * 2, moved=half * width * 20
            )(keep, got)
            got = exchange(send, "head", head_count, flip)
        return keep, got

    def block(layer, raw, ready, qkv, out, extra):
        half = blocks // 2 * rows
        return call(
            functools.partial(
                block_kernel,
                (heads, 2 * rows if layer else rows, 2 * piece_rows if layer else piece_rows, layer, len(raw), len(ready)),
            ),
            (shape((half, width), BF16), shape((half, width), F32)),
            [VMEM] * (len(raw) + len(ready) + 3 + len(extra)),
            [pltpu.VMEM((blocks * rows, width), BF16), pltpu.VMEM((3 * heads, dim, blocks * rows), BF16),
             pltpu.VMEM((depth, blocks * rows), BF16)],
            flops=2 * blocks * rows * (heads * triple + depth) * width,
            moved=qkv.size * 2,
        )(*raw, *ready, gains, qkv, out, *extra)

    qkv = qkv_weight.transpose(0, 2, 3, 1).reshape(2, heads * triple, width)
    table = time_table.transpose(1, 0, 2)
    shift = shift_table.transpose(1, 0, 2)

    held = spread(own, flips)
    pair = exchange(own, "sub", sub_count, 1)
    mods, gains, normed, mine, qkv0, qkv1, out0, out1 = call(
        functools.partial(first_kernel, piece_rows),
        (shape((8, width), F32), shape((4, dim, 1), F32), shape((rows, width), BF16), shape((rows, width), BF16),
         shape(qkv.shape[1:], BF16), shape(qkv.shape[1:], BF16), shape((depth, width), BF16), shape((depth, width), BF16)),
        [SMEM] + [HBM] * 6,
        [pltpu.VMEM(table.shape, F32), pltpu.VMEM(shift.shape, F32),
         pltpu.VMEM(norm_gains.shape, F32), pltpu.VMEM(own.shape, BF16), pltpu.SemaphoreType.DMA((8,))],
        flops=10**9,
        moved=qkv.size * 2,
    )(timestep, in_hbm(table), in_hbm(shift), in_hbm(own), in_hbm(norm_gains), in_hbm(qkv), in_hbm(out_weight))

    far = [held[j] for j in sorted(held) if j]
    far, mods = lax.optimization_barrier((far, mods))
    fresh = [exchange(value, "sub", sub_count, 1) for value in far]
    theirs, near = call(
        functools.partial(prepare_kernel, piece_rows, 1 + len(far)),
        (shape((rows, width), BF16), shape(((1 + len(far)) * rows, width), BF16)),
        [VMEM] * (2 + len(far)),
        flops=5 * 10**8,
        moved=rows * width * 8,
    )(mods, pair, *far)
    send, keep = block(0, fresh, [normed, near], qkv0, out0, [mods])

    keep, got = reduce(send, keep, flips[1:])
    near, distant, kept = call(
        split_kernel,
        (shape((rows, width), BF16), shape((rows, width), BF16), shape((2 * rows, width), F32)),
        [VMEM] * 2,
        moved=rows * width * 20,
    )(keep, got)
    distant = exchange(distant, "head", head_count, 1)
    near = exchange(near, "head", head_count, 1)
    middle = seq_count // 2

    def half_block(start, got, *after):
        return call(
            functools.partial(middle_kernel, start, piece_rows),
            (shape((rows // 2, width), BF16),) + (shape((2 * piece_rows, width), BF16),) * middle,
            [VMEM] * (5 + len(after)),
            moved=rows * width * 16,
        )(kept, got, mine, theirs, mods, *after)

    current_far, *pieces_far = half_block(rows // 2, distant)
    moved = {k: exchange(pieces_far[k - middle], "seq", seq_count, k) for k in reversed(range(middle, seq_count))}
    current_near, *pieces_near = half_block(0, near, current_far)
    moved.update({k: exchange(pieces_near[k], "seq", seq_count, k) for k in reversed(range(1, middle))})
    moved[0] = pieces_near[0]
    tokens = jnp.concatenate([moved[k] for k in range(seq_count)], axis=0)

    held = spread(tokens, flips[1:])
    for j in list(held):
        held[j | 1] = exchange(held[j], "sub", sub_count, 1)
    send, keep = block(1, [], [held[j] for j in sorted(held)], qkv1, out1, [])

    keep, got = reduce(send, keep, flips[1:])
    send, keep = call(
        functools.partial(merge_kernel, seq_count),
        (shape((rows, width), BF16), shape((rows, width), F32)),
        [VMEM] * 2,
        moved=rows * width * 20,
    )(keep, got)
    got = exchange(send, "head", head_count, 1)
    pieces = call(
        functools.partial(finish_kernel, seq_count),
        (shape((piece_rows, width), BF16),) * seq_count,
        [VMEM] * 2,
        moved=rows * width * 8,
    )(keep, got)
    back = {k: exchange(pieces[k], "seq", seq_count, k) for k in reversed(range(1, seq_count))}
    back[0] = pieces[0]
    return call(
        functools.partial(last_kernel, seq_count),
        jax.ShapeDtypeStruct((1, rows, width), BF16),
        [VMEM] * (3 + seq_count),
        [pltpu.VMEM((rows, width), BF16)],
        moved=rows * width * 8,
    )(current_near, current_far, mods, *[back[k] for k in range(seq_count)])


def solution(mesh):
    seq_count = mesh.shape["seq"]

    def named(*args):
        return body(mesh.shape["head"], mesh.shape["sub"], seq_count, *args)

    return jax.shard_map(
        named,
        mesh=mesh,
        in_specs=(
            P(("grp", "seq"), ("head", "sub"), None),
            P("grp"),
            P(),
            P(),
            P(None, None, ("head", "sub"), None),
            P(),
            P(None, ("head", "sub"), None),
        ),
        out_specs=P(("grp", "seq"), ("head", "sub"), None),
        check_vma=False,
    )
```
